256 devices in a mesh: mom: 64 (over z, y, core), idx: 4 (over x).
Axes of the slice: x: 4, y: 4, z: 8, core: 2. Of those that a mesh axis runs over, the one named last changes fastest.
Arguments:
- vertex: bfloat16 [3, 256, 512, 512], P(None, 'mom', None, 'idx'), may hold values from -0.25 to 0.25
- formfactors: bfloat16 [2048, 512], replicated, may hold values from -6 to 6
- propagator: float32 [256], replicated, may hold values from -4 to 4
- loop_mom: int32 [2048], replicated, may hold values from 0 to 255
- bond_disp: int32 [8, 2], replicated, may hold values from 0 to 15
- proj_channel: int32 [3, 8, 4], replicated, may hold values from 0 to 2
- proj_bond: int32 [3, 8, 4], replicated, may hold values from 0 to 7
- proj_phase: int32 [3, 8, 4], replicated, may hold values from 0 to 3
Outputs:
- flow: float32 [3, 256, 512, 512], P(None, 'mom', None, 'idx')
The draws below stay inside these ranges and needn't reach their ends.
All inputs are finite; a program needn't handle non-finite values.
Results may differ from the reference program's by a relative error of at most 0.005.
Values may be sent and summed in bfloat16 or wider, within the bound.
No kernel may reach another device: no remote copies, remote signals or barrier semaphores. Data moves between devices by JAX's collectives and lax.ppermute only.
A program may use at most 128 MiB of HBM per device.

```python
import math
import jax
import jax.numpy as jnp
from jax import lax

MSIDE = 16
NQ = 256
NI = 512
NL = 2048
NB = 8
SOURCES = 4


def place_ends(entries, stream_key, low, top_value):
    longest = entries.shape.index(max(entries.shape))
    spots = []
    for shift in (0, 1):
        where = [jax.random.randint(jax.random.fold_in(stream_key, axis), (), 0, length) for axis, length in enumerate(entries.shape)]
        where[longest] = (where[longest] + shift) % entries.shape[longest]
        spots.append(tuple(where))
    return entries.at[spots[0]].set(low).at[spots[1]].set(top_value)


def steps_of(rng, extent, split, least, largest):
    def one(position, shards_of):
        steps = jax.random.uniform(jax.random.fold_in(jax.random.fold_in(rng, 6), position), (shards_of,), jnp.float32, least / len(split), largest / len(split))
        return jnp.repeat(jnp.exp(steps), extent[position] // shards_of).reshape((-1,) + (1,) * (len(extent) - position - 1))

    factor_of = one(*split[0])
    for cut in split[1:]:
        factor_of = factor_of * one(*cut)
    return factor_of


def scatter_about(rng, shape, width, most, pieces=(), kind=jnp.bfloat16):
    entries = width * jax.random.normal(rng, shape, jnp.float32)
    if pieces:
        entries = entries * steps_of(rng, shape, pieces, -0.22, 0.18)
    return jnp.clip(entries, -most, most).astype(kind)


def setup_inputs(seed: int = 0) -> dict:
    key_list = jax.random.split(jax.random.key(seed), 9)
    vertex = scatter_about(key_list[0], (3, NQ, NI, NI), NI ** -0.5, 0.25, ((1, 64), (3, 4)))
    formfactors = scatter_about(key_list[1], (NL, NI), 1.0, 6.0)
    propagator = scatter_about(key_list[2], (NQ,), 1.0, 4.0, (), jnp.float32)
    loop_mom = place_ends(jax.random.randint(key_list[3], (NL,), 0, NQ), jax.random.fold_in(key_list[3], 1), 0, NQ - 1).astype(jnp.int32)
    bond_disp = place_ends(jax.random.randint(key_list[4], (NB, 2), 0, MSIDE), jax.random.fold_in(key_list[4], 1), 0, MSIDE - 1).astype(jnp.int32)
    proj_channel = place_ends(jax.random.randint(key_list[5], (3, NB, SOURCES), 0, 3), jax.random.fold_in(key_list[5], 1), 0, 2).astype(jnp.int32)
    proj_bond = place_ends(jax.random.randint(key_list[6], (3, NB, SOURCES), 0, NB), jax.random.fold_in(key_list[6], 1), 0, NB - 1).astype(jnp.int32)
    proj_phase = place_ends(jax.random.randint(key_list[7], (3, NB, SOURCES), 0, 4), jax.random.fold_in(key_list[7], 1), 0, 3).astype(jnp.int32)
    return dict(vertex=vertex, formfactors=formfactors, propagator=propagator, loop_mom=loop_mom, bond_disp=bond_disp, proj_channel=proj_channel, proj_bond=proj_bond, proj_phase=proj_phase)


def momentum_sum(former, latter, signed):
    coord_x = (former // MSIDE + signed * (latter // MSIDE)) % MSIDE
    coord_y = (former % MSIDE + signed * (latter % MSIDE)) % MSIDE
    return (coord_x * MSIDE + coord_y).astype(jnp.int32)

def loop_weights(propagator, loop_mom, momenta):
    pair = momentum_sum(momenta[:, None], loop_mom[None, :], -1)
    plus = momentum_sum(loop_mom[None, :], momenta[:, None], 1)
    minus = momentum_sum(loop_mom[None, :], momenta[:, None], -1)
    own = propagator[loop_mom][None, :]
    return jnp.stack([own * propagator[pair], own * propagator[plus], own * propagator[minus]])

def phase_table(bond_disp, momenta):
    coord_x = momenta // MSIDE
    coord_y = momenta % MSIDE
    turns = (bond_disp[:, 0:1] * coord_x[None, :] + bond_disp[:, 1:2] * coord_y[None, :]) % MSIDE
    angles = turns.astype(jnp.float32) * (2.0 * math.pi / MSIDE)
    return jnp.stack([jnp.cos(angles), -jnp.sin(angles)]).astype(jnp.bfloat16)

def mixing_tables(proj_channel, proj_bond, proj_phase):
    chan_hot = (proj_channel[..., None] == jnp.arange(3, dtype=jnp.int32)).astype(jnp.float32)
    bond_hot = (proj_bond[..., None] == jnp.arange(proj_bond.shape[1], dtype=jnp.int32)).astype(jnp.float32)
    direct = (proj_phase == 0).astype(jnp.float32) - (proj_phase == 2).astype(jnp.float32)
    crossed = (proj_phase == 3).astype(jnp.float32) - (proj_phase == 1).astype(jnp.float32)
    same = jnp.einsum('xysu,xysv,xys->xyuv', chan_hot, bond_hot, direct, precision=lax.Precision.HIGHEST)
    swapped = jnp.einsum('xysu,xysv,xys->xyuv', chan_hot, bond_hot, crossed, precision=lax.Precision.HIGHEST)
    return (same, swapped)

def reference(vertex, formfactors, propagator, loop_mom, bond_disp, proj_channel, proj_bond, proj_phase):
    momenta = jnp.arange(NQ, dtype=jnp.int32)
    weights = loop_weights(propagator, loop_mom, momenta)
    scale_nl = 1.0 / math.sqrt(NL)
    form_wide = formfactors.astype(jnp.float32)

    def per_momentum(index):
        vertex_q = lax.dynamic_index_in_dim(vertex, index, 1, keepdims=False).astype(jnp.float32)
        weight_q = lax.dynamic_index_in_dim(weights, index, 1, keepdims=False)
        loop_terms = jnp.einsum('li,cij->clj', form_wide, vertex_q, precision=lax.Precision.HIGHEST)
        weighted = (loop_terms * weight_q[:, :, None] * scale_nl).astype(jnp.bfloat16)
        weighted = lax.optimization_barrier(weighted).astype(jnp.float32)
        kernel = jnp.einsum('li,clj->cij', form_wide, weighted, precision=lax.Precision.HIGHEST).astype(jnp.bfloat16)
        kernel = lax.optimization_barrier(kernel).astype(jnp.float32)
        return jnp.einsum('cia,caj->cij', vertex_q, kernel, precision=lax.Precision.HIGHEST)
    increment = lax.map(per_momentum, momenta)
    increment_b = lax.optimization_barrier(increment.astype(jnp.bfloat16)).astype(jnp.float32)
    phases = phase_table(bond_disp, momenta).astype(jnp.float32)
    bond_terms = jnp.einsum('pbq,qcij->icpbj', phases, increment_b, precision=lax.Precision.HIGHEST) * (1.0 / MSIDE)
    same, swapped = mixing_tables(proj_channel, proj_bond, proj_phase)
    real_part = bond_terms[:, :, 0]
    imag_part = bond_terms[:, :, 1]

    def mixing(table, values):
        return jnp.einsum('xyuv,iuvj->ixyj', table, values, precision=lax.Precision.HIGHEST)
    proj_real = mixing(same, real_part) + mixing(swapped, imag_part)
    proj_imag = mixing(same, imag_part) - mixing(swapped, real_part)
    projected = jnp.stack([proj_real, proj_imag], axis=2).astype(jnp.bfloat16)
    projected = lax.optimization_barrier(projected).astype(jnp.float32)
    back_scale = 1.0 / math.sqrt(NB * SOURCES)
    returned = jnp.einsum('pbq,icpbj->qcij', phases, projected, precision=lax.Precision.HIGHEST) * back_scale
    flow = increment + returned
    return jnp.moveaxis(flow, 0, 1)
```

```python
import math

import jax
import jax.numpy as jnp
from jax import lax
from jax.experimental import pallas as pl
from jax.experimental.pallas import tpu as pltpu
from jax.sharding import Mesh
from jax.sharding import PartitionSpec as P

MSIDE = 16
NQ = 256
NI = 512
NL = 2048
NB = 8
SOURCES = 4
COLS = 128
GROUP = 64
OWNERS = 16
ROWS = NI // OWNERS
QUARTER = ROWS // 4
LCHUNK = 512


BF = jnp.bfloat16
F32 = jnp.float32


def cost(flops, nbytes):
    return pl.CostEstimate(flops=flops, bytes_accessed=nbytes, transcendentals=0)


def nt_dot(a, b):
    return lax.dot_general(a, b, (((1,), (1,)), ((), ())), preferred_element_type=F32)


def momentum_sum(former, latter, signed):
    coord_x = (former // MSIDE + signed * (latter // MSIDE)) % MSIDE
    coord_y = (former % MSIDE + signed * (latter % MSIDE)) % MSIDE
    return coord_x * MSIDE + coord_y


def lookup(values, indices):
    hits = indices[..., None] == jnp.arange(values.shape[0], dtype=jnp.int32)
    return jnp.sum(jnp.where(hits, values, 0.0), axis=-1)


def loop_weights(propagator, loop_mom, q):
    every = jnp.arange(NQ, dtype=jnp.int32)
    partners = jnp.stack(
        [momentum_sum(q, every, -1), momentum_sum(every, q, 1), momentum_sum(every, q, -1)]
    )
    table = jnp.concatenate([propagator[None, :], lookup(propagator, partners)], axis=0)
    hot = (every[:, None] == loop_mom[None, :]).astype(F32)
    found = jnp.einsum("nk,kl->nl", table, hot, precision=lax.Precision.HIGHEST)
    return found[0:1] * found[1:4] * (1.0 / math.sqrt(NL))


def phase_table(bond_disp, momenta):
    coord_x = momenta // MSIDE
    coord_y = momenta % MSIDE
    turns = (bond_disp[:, 0:1] * coord_x[None, :] + bond_disp[:, 1:2] * coord_y[None, :]) % MSIDE
    angles = turns.astype(F32) * (2.0 * math.pi / MSIDE)
    return jnp.concatenate([jnp.cos(angles), -jnp.sin(angles)], axis=0).astype(BF)


def spread(count, each):
    long = lax.broadcasted_iota(jnp.int32, (count * each, count), 0) // each
    short = lax.broadcasted_iota(jnp.int32, (count * each, count), 1)
    return (long == short).astype(BF)


def times_identity(matrix, each):
    rows, cols = matrix.shape
    wide = jnp.einsum("rc,kc->rk", matrix, spread(cols, each), preferred_element_type=F32)
    full = jnp.einsum(
        "mr,rk->mk", spread(rows, each), wide.astype(BF), preferred_element_type=F32
    )
    row_id = lax.broadcasted_iota(jnp.int32, full.shape, 0) % each
    col_id = lax.broadcasted_iota(jnp.int32, full.shape, 1) % each
    return jnp.where(row_id == col_id, full, 0.0)


def mixing_matrix(proj_channel, proj_bond, proj_phase):
    chan_hot = (proj_channel[..., None] == jnp.arange(3, dtype=jnp.int32)).astype(F32)
    bond_hot = (proj_bond[..., None] == jnp.arange(NB, dtype=jnp.int32)).astype(F32)
    direct = (proj_phase == 0).astype(F32) - (proj_phase == 2).astype(F32)
    crossed = (proj_phase == 3).astype(F32) - (proj_phase == 1).astype(F32)
    pair = (bond_hot[..., :, None] * chan_hot[..., None, :]).reshape(3, NB, SOURCES, 3 * NB)
    same = jnp.sum(pair * direct[..., None], axis=2)
    swapped = jnp.sum(pair * crossed[..., None], axis=2)
    same = jnp.swapaxes(same, 0, 1).reshape(3 * NB, 3 * NB)
    swapped = jnp.swapaxes(swapped, 0, 1).reshape(3 * NB, 3 * NB)
    upper = jnp.concatenate([same, swapped], axis=1)
    lower = jnp.concatenate([-swapped, same], axis=1)
    return (jnp.concatenate([upper, lower], axis=0) * (1.0 / MSIDE)).astype(BF)


def kernel_rows(panels, form, turned_form, weights, total):
    turned = jnp.concatenate([panel(c).T for panel in panels for c in range(3)], axis=0)
    count = 3 * len(panels)
    for step in range(NL // LCHUNK):
        low, high = step * LCHUNK, (step + 1) * LCHUNK
        terms = jnp.dot(turned, turned_form[:, low:high], preferred_element_type=F32)
        weighted = jnp.concatenate(
            [
                (
                    terms[k * COLS : (k + 1) * COLS] * weights[k % 3 : k % 3 + 1, low:high]
                ).astype(BF)
                for k in range(count)
            ],
            axis=0,
        )
        add = jnp.dot(weighted, form[low:high, :], preferred_element_type=F32)
        if step == 0:
            total[...] = add
        else:
            total[...] += add


def own_body(place, vertex, form, turned_form, weights, out, total):
    kernel_rows([lambda c: vertex[c, 0]], form, turned_form, weights, total)
    out[...] = total[...].astype(BF)


def panel_body(panel, form, turned_form, weights, out, total):
    kernel_rows([lambda c: panel[c]], form, turned_form, weights, total)
    out[...] = total[...].astype(BF)


def last_body(
    place, vertex, v1, v2, v3, form, turned_form, weights, k0, k2, out, total, whole, k13
):
    x = place[0]
    kernel_rows([lambda c: v1[c], lambda c: v3[c]], form, turned_form, weights, total)
    k13[...] = total[...].astype(BF)
    for c in range(3):
        for s in range(4):
            piece = vertex[c, 0] if s == 0 else (v1, v2, v3)[s - 1][c]
            whole[c, lax.rem(x + 4 - s, 4)] = piece
    for c in range(3):
        row = c * COLS
        natural = jnp.concatenate([whole[c, n] for n in range(4)], axis=1)
        rows = jnp.concatenate(
            [
                k0[row : row + COLS],
                k13[row : row + COLS],
                k2[row : row + COLS],
                k13[3 * COLS + row : 3 * COLS + row + COLS],
            ],
            axis=0,
        )
        inc = nt_dot(natural, rows).astype(BF)
        for s in range(4):
            part = inc[:, s * COLS : (s + 1) * COLS].reshape(OWNERS, 1, ROWS, COLS)
            out[:, pl.ds(lax.rem(x + 4 - s, 4), 1), c] = part


VM = pl.BlockSpec(memory_space=pltpu.VMEM)
SMALL = pltpu.CompilerParams(vmem_limit_bytes=24 << 20)
KERNEL_FLOPS = 2 * 2 * 3 * COLS * NL * NI


def own_spec():
    return pl.BlockSpec((3, 1, NI, COLS), lambda i, place: (0, place[0], 0, 0))


def whole_spec(shape):
    return pl.BlockSpec(shape, lambda i, place: (0,) * len(shape))


def own_rows(place, vertex, form, turned_form, weights):
    return pl.pallas_call(
        own_body,
        out_shape=jax.ShapeDtypeStruct((3 * COLS, NI), BF),
        grid_spec=pltpu.PrefetchScalarGridSpec(
            num_scalar_prefetch=1,
            grid=(1,),
            in_specs=[
                own_spec(),
                whole_spec((NL, NI)),
                whole_spec((NI, NL)),
                whole_spec((3, NL)),
            ],
            out_specs=whole_spec((3 * COLS, NI)),
            scratch_shapes=[pltpu.VMEM((3 * COLS, NI), F32)],
        ),
        cost_estimate=cost(KERNEL_FLOPS, 3 << 20),
        compiler_params=SMALL,
        name="own_rows",
    )(place, vertex, form, turned_form, weights)


def panel_rows(panel, form, turned_form, weights):
    return pl.pallas_call(
        panel_body,
        out_shape=jax.ShapeDtypeStruct((3 * COLS, NI), BF),
        in_specs=[VM] * 4,
        out_specs=VM,
        scratch_shapes=[pltpu.VMEM((3 * COLS, NI), F32)],
        cost_estimate=cost(KERNEL_FLOPS, 3 << 20),
        compiler_params=SMALL,
        name="panel_rows",
    )(panel, form, turned_form, weights)


def last_rows(place, vertex, v1, v2, v3, form, turned_form, weights, k0, k2):
    panel = whole_spec((3, NI, COLS))
    rows = whole_spec((3 * COLS, NI))
    return pl.pallas_call(
        last_body,
        out_shape=jax.ShapeDtypeStruct((OWNERS, 4, 3, ROWS, COLS), BF),
        grid_spec=pltpu.PrefetchScalarGridSpec(
            num_scalar_prefetch=1,
            grid=(1,),
            in_specs=[
                own_spec(),
                panel,
                panel,
                panel,
                whole_spec((NL, NI)),
                whole_spec((NI, NL)),
                whole_spec((3, NL)),
                rows,
                rows,
            ],
            out_specs=whole_spec((OWNERS, 4, 3, ROWS, COLS)),
            scratch_shapes=[
                pltpu.VMEM((6 * COLS, NI), F32),
                pltpu.VMEM((3, 4, NI, COLS), BF),
                pltpu.VMEM((6 * COLS, NI), BF),
            ],
        ),
        cost_estimate=cost(2 * KERNEL_FLOPS + 2 * 3 * NI * NI * NI, 8 << 20),
        compiler_params=pltpu.CompilerParams(vmem_limit_bytes=36 << 20),
        name="last_rows",
    )(place, vertex, v1, v2, v3, form, turned_form, weights, k0, k2)


def forward_body(terms, matrix, out):
    for c in range(3):
        row = c * ROWS
        halves = [terms[:, row + h : row + h + 16, :].reshape(GROUP * 16, COLS) for h in (0, 16)]
        both = jnp.concatenate(halves, axis=1)
        part = jnp.dot(matrix[...], both, preferred_element_type=F32).astype(BF)
        for half in range(2):
            one = part[:, half * COLS : (half + 1) * COLS].reshape(2 * NB, 16, COLS)
            out[2 * half, :, c] = one[:, :QUARTER]
            out[2 * half + 1, :, c] = one[:, QUARTER:]


BONDS = (2 * NB, 3, QUARTER, COLS)


def forward(terms, matrix):
    return pl.pallas_call(
        forward_body,
        out_shape=jax.ShapeDtypeStruct((4,) + BONDS, BF),
        in_specs=[VM, VM],
        out_specs=VM,
        cost_estimate=cost(2 * 256 * 1024 * 768, 3 << 20),
        compiler_params=SMALL,
        name="forward",
    )(terms, matrix)


def mix_body(parts, matrix, out):
    total = parts[0].astype(F32)
    for k in range(1, 4):
        total += parts[k].astype(F32)
    flat = total.reshape(6 * NB * QUARTER, COLS)
    high = flat.astype(BF)
    rest = flat - high.astype(F32)
    middle = rest.astype(BF)
    low = (rest - middle.astype(F32)).astype(BF)
    split = jnp.concatenate([high, middle, low], axis=1)
    mixed = jnp.dot(matrix[...], split, preferred_element_type=F32)
    mixed = mixed[:, :COLS] + (mixed[:, COLS : 2 * COLS] + mixed[:, 2 * COLS :])
    out[...] = mixed.reshape(BONDS).astype(BF)


def mix(parts, matrix):
    return pl.pallas_call(
        mix_body,
        out_shape=jax.ShapeDtypeStruct(BONDS, BF),
        in_specs=[VM] * 2,
        out_specs=VM,
        cost_estimate=cost(2 * 384 * 384 * 384, 1 << 20),
        compiler_params=SMALL,
        name="mix",
    )(parts, matrix)


def backward_body(parts, terms, matrix, out):
    scale = 1.0 / math.sqrt(NB * SOURCES)
    for c in range(3):
        row = c * ROWS
        halves = [
            jnp.concatenate([parts[2 * h, :, c], parts[2 * h + 1, :, c]], axis=1).reshape(
                2 * NB * 16, COLS
            )
            for h in range(2)
        ]
        back = jnp.dot(
            matrix[...], jnp.concatenate(halves, axis=1), preferred_element_type=F32
        )
        for half in range(2):
            here = row + half * 16
            one = back[:, half * COLS : (half + 1) * COLS].reshape(GROUP, 16, COLS)
            flow = terms[:, here : here + 16, :].astype(F32) + one * scale
            out[:, here : here + 16, :] = flow.astype(BF)


def backward(parts, terms, matrix):
    return pl.pallas_call(
        backward_body,
        out_shape=jax.ShapeDtypeStruct((GROUP, 3 * ROWS, COLS), BF),
        in_specs=[VM] * 3,
        out_specs=VM,
        cost_estimate=cost(2 * 256 * 1024 * 768, 5 << 20),
        compiler_params=SMALL,
        name="backward",
    )(parts, terms, matrix)


def finish_body(pieces, out):
    for w in range(OWNERS):
        out[0, 0, w * ROWS : (w + 1) * ROWS, :] = pieces[w, 0, 0].astype(F32)


def finish(pieces):
    return pl.pallas_call(
        finish_body,
        out_shape=jax.ShapeDtypeStruct((3, 4, NI, COLS), F32),
        grid=(3, 4),
        in_specs=[pl.BlockSpec((OWNERS, 1, 1, ROWS, COLS), lambda c, r: (0, r, c, 0, 0))],
        out_specs=pl.BlockSpec((1, 1, NI, COLS), lambda c, r: (c, r, 0, 0)),
        cost_estimate=cost(1 << 20, 5 << 20),
        compiler_params=SMALL,
        name="finish",
    )(pieces)


def turn(value, axis, shift):
    return lax.ppermute(value, axis, [(k, (k + shift) % 4) for k in range(4)])


def local(
    vertex, formfactors, propagator, loop_mom, bond_disp, proj_channel, proj_bond, proj_phase
):
    x = lax.axis_index("x")
    z = lax.axis_index("z4")
    owner = lax.axis_index(("z4", "z2", "y", "c"))
    place_x = jnp.reshape(x, (1,)).astype(jnp.int32)

    sent = [lax.dynamic_index_in_dim(vertex, (x + s) % 4, 1, keepdims=False) for s in (1, 2, 3)]
    v1, v2, v3 = (turn(piece, "x", s) for s, piece in zip((1, 2, 3), sent))

    weights = loop_weights(propagator, loop_mom, 4 * owner + x)
    turned_form = formfactors.T
    phases = phase_table(bond_disp, GROUP * z + jnp.arange(GROUP, dtype=jnp.int32))
    there = times_identity(phases, 16).astype(BF)
    back = times_identity(phases.T, 16).astype(BF)
    mixing = mixing_matrix(proj_channel, proj_bond, proj_phase)
    mixing = times_identity(mixing, QUARTER).astype(BF)

    k0 = own_rows(place_x, vertex, formfactors, turned_form, weights)
    k2 = panel_rows(v2, formfactors, turned_form, weights)
    increment = last_rows(
        place_x, vertex, v1, v2, v3, formfactors, turned_form, weights, k0, k2
    )
    increment = increment.reshape(GROUP, 3 * ROWS, COLS)
    terms = lax.all_to_all(increment, ("z2", "y", "c", "x"), 0, 0, tiled=True)

    sums = lax.all_to_all(forward(terms, there), "z4", 0, 0, tiled=True)
    parts = lax.all_gather(mix(sums, mixing), "z4", axis=0, tiled=False)
    flow = backward(parts, terms, back)
    flow = flow.reshape(OWNERS, 4 * 3 * ROWS, COLS)
    pieces = lax.all_to_all(flow, ("z2", "y", "c"), 0, 0, tiled=True)
    return finish(pieces.reshape(OWNERS, 4, 3, ROWS, COLS))


def solution(mesh):
    fine = Mesh(mesh.devices.reshape(4, 2, 4, 2, 4), ("z4", "z2", "y", "c", "x"))
    placed = P(None, ("z4", "z2", "y", "c"), None, "x")
    in_specs = (placed, P(), P(), P(), P(), P(), P(), P())
    return jax.shard_map(local, mesh=fine, in_specs=in_specs, out_specs=placed, check_vma=False)
```

```python
import math

import jax
import jax.numpy as jnp
from jax import lax
from jax.experimental import pallas as pl
from jax.experimental.pallas import tpu as pltpu
from jax.sharding import Mesh
from jax.sharding import PartitionSpec as P

MSIDE = 16
NQ = 256
NI = 512
NL = 2048
NB = 8
SOURCES = 4
COLS = 128
GROUP = 64
OWNERS = 16
ROWS = NI // OWNERS
QUARTER = ROWS // 4
LCHUNK = 512


BF = jnp.bfloat16
F32 = jnp.float32


def cost(flops, nbytes):
    return pl.CostEstimate(flops=flops, bytes_accessed=nbytes, transcendentals=0)


def nt_dot(a, b):
    return lax.dot_general(a, b, (((1,), (1,)), ((), ())), preferred_element_type=F32)


def momentum_sum(former, latter, signed):
    coord_x = (former // MSIDE + signed * (latter // MSIDE)) % MSIDE
    coord_y = (former % MSIDE + signed * (latter % MSIDE)) % MSIDE
    return coord_x * MSIDE + coord_y


def lookup(values, indices):
    hits = indices[..., None] == jnp.arange(values.shape[0], dtype=jnp.int32)
    return jnp.sum(jnp.where(hits, values, 0.0), axis=-1)


def loop_weights(propagator, loop_mom, q):
    every = jnp.arange(NQ, dtype=jnp.int32)
    partners = jnp.stack(
        [momentum_sum(q, every, -1), momentum_sum(every, q, 1), momentum_sum(every, q, -1)]
    )
    table = jnp.concatenate([propagator[None, :], lookup(propagator, partners)], axis=0)
    hot = (every[:, None] == loop_mom[None, :]).astype(F32)
    found = jnp.einsum("nk,kl->nl", table, hot, precision=lax.Precision.HIGHEST)
    return found[0:1] * found[1:4] * (1.0 / math.sqrt(NL))


def phase_table(bond_disp, momenta):
    coord_x = momenta // MSIDE
    coord_y = momenta % MSIDE
    turns = (bond_disp[:, 0:1] * coord_x[None, :] + bond_disp[:, 1:2] * coord_y[None, :]) % MSIDE
    angles = turns.astype(F32) * (2.0 * math.pi / MSIDE)
    return jnp.concatenate([jnp.cos(angles), -jnp.sin(angles)], axis=0).astype(BF)


def spread(count, each):
    long = lax.broadcasted_iota(jnp.int32, (count * each, count), 0) // each
    short = lax.broadcasted_iota(jnp.int32, (count * each, count), 1)
    return (long == short).astype(BF)


def times_identity(matrix, each):
    rows, cols = matrix.shape
    wide = jnp.einsum("rc,kc->rk", matrix, spread(cols, each), preferred_element_type=F32)
    full = jnp.einsum(
        "mr,rk->mk", spread(rows, each), wide.astype(BF), preferred_element_type=F32
    )
    row_id = lax.broadcasted_iota(jnp.int32, full.shape, 0) % each
    col_id = lax.broadcasted_iota(jnp.int32, full.shape, 1) % each
    return jnp.where(row_id == col_id, full, 0.0)


def mixing_matrix(proj_channel, proj_bond, proj_phase):
    chan_hot = (proj_channel[..., None] == jnp.arange(3, dtype=jnp.int32)).astype(F32)
    bond_hot = (proj_bond[..., None] == jnp.arange(NB, dtype=jnp.int32)).astype(F32)
    direct = (proj_phase == 0).astype(F32) - (proj_phase == 2).astype(F32)
    crossed = (proj_phase == 3).astype(F32) - (proj_phase == 1).astype(F32)
    pair = (bond_hot[..., :, None] * chan_hot[..., None, :]).reshape(3, NB, SOURCES, 3 * NB)
    same = jnp.sum(pair * direct[..., None], axis=2)
    swapped = jnp.sum(pair * crossed[..., None], axis=2)
    same = jnp.swapaxes(same, 0, 1).reshape(3 * NB, 3 * NB)
    swapped = jnp.swapaxes(swapped, 0, 1).reshape(3 * NB, 3 * NB)
    upper = jnp.concatenate([same, swapped], axis=1)
    lower = jnp.concatenate([-swapped, same], axis=1)
    return (jnp.concatenate([upper, lower], axis=0) * (1.0 / MSIDE)).astype(BF)


def kernel_rows(panels, form, turned_form, weights, total):
    turned = jnp.concatenate([panel(c).T for panel in panels for c in range(3)], axis=0)
    count = 3 * len(panels)
    for step in range(NL // LCHUNK):
        low, high = step * LCHUNK, (step + 1) * LCHUNK
        terms = jnp.dot(turned, turned_form[:, low:high], preferred_element_type=F32)
        weighted = jnp.concatenate(
            [
                (
                    terms[k * COLS : (k + 1) * COLS] * weights[k % 3 : k % 3 + 1, low:high]
                ).astype(BF)
                for k in range(count)
            ],
            axis=0,
        )
        add = jnp.dot(weighted, form[low:high, :], preferred_element_type=F32)
        if step == 0:
            total[...] = add
        else:
            total[...] += add


def own_body(place, vertex, form, weights, out, turned_form, v0, total, sem):
    own = pltpu.make_async_copy(vertex.at[:, place[0]], v0, sem)
    own.start()
    for step in range(NL // LCHUNK):
        low, high = step * LCHUNK, (step + 1) * LCHUNK
        turned_form[:, low:high] = form[low:high, :].T
    own.wait()
    kernel_rows([lambda c: v0[c]], form, turned_form, weights, total)
    out[...] = total[...].astype(BF)


def panel_body(panel, form, turned_form, weights, out, total):
    kernel_rows([lambda c: panel[c]], form, turned_form, weights, total)
    out[...] = total[...].astype(BF)


def last_body(
    place, v0, v1, v2, v3, form, turned_form, weights, k0, k2, out, total, whole, k13, held, sems
):
    x = place[0]
    kernel_rows([lambda c: v1[c], lambda c: v3[c]], form, turned_form, weights, total)
    k13[...] = total[...].astype(BF)
    for c in range(3):
        for s in range(4):
            whole[c, lax.rem(x + 4 - s, 4)] = (v0, v1, v2, v3)[s][c]

    def copy(c):
        return pltpu.make_async_copy(held.at[c], out.at[:, :, c], sems.at[c])

    for c in range(3):
        row = c * COLS
        natural = jnp.concatenate([whole[c, n] for n in range(4)], axis=1)
        rows = jnp.concatenate(
            [
                k0[row : row + COLS],
                k13[row : row + COLS],
                k2[row : row + COLS],
                k13[3 * COLS + row : 3 * COLS + row + COLS],
            ],
            axis=0,
        )
        inc = nt_dot(natural, rows).astype(BF)
        for s in range(4):
            part = inc[:, s * COLS : (s + 1) * COLS].reshape(OWNERS, 1, ROWS, COLS)
            held[c, :, pl.ds(lax.rem(x + 4 - s, 4), 1)] = part
        if c > 0:
            copy(c - 1).start()
    copy(2).start()
    for c in range(3):
        copy(c).wait()


VM = pl.BlockSpec(memory_space=pltpu.VMEM)
SMALL = pltpu.CompilerParams(vmem_limit_bytes=24 << 20)
KERNEL_FLOPS = 2 * 2 * 3 * COLS * NL * NI


HB = pl.BlockSpec(memory_space=pltpu.HBM)
SM = pl.BlockSpec(memory_space=pltpu.SMEM)


def own_rows(place, vertex, form, weights):
    return pl.pallas_call(
        own_body,
        out_shape=[
            jax.ShapeDtypeStruct((3 * COLS, NI), BF),
            jax.ShapeDtypeStruct((NI, NL), BF),
            jax.ShapeDtypeStruct((3, NI, COLS), BF),
        ],
        in_specs=[SM, HB, VM, VM],
        out_specs=[VM] * 3,
        scratch_shapes=[pltpu.VMEM((3 * COLS, NI), F32), pltpu.SemaphoreType.DMA],
        cost_estimate=cost(KERNEL_FLOPS, 3 << 20),
        compiler_params=SMALL,
        name="own_rows",
    )(place, vertex, form, weights)


def panel_rows(panel, form, turned_form, weights):
    return pl.pallas_call(
        panel_body,
        out_shape=jax.ShapeDtypeStruct((3 * COLS, NI), BF),
        in_specs=[VM] * 4,
        out_specs=VM,
        scratch_shapes=[pltpu.VMEM((3 * COLS, NI), F32)],
        cost_estimate=cost(KERNEL_FLOPS, 3 << 20),
        compiler_params=SMALL,
        name="panel_rows",
    )(panel, form, turned_form, weights)


def last_rows(place, v0, v1, v2, v3, form, turned_form, weights, k0, k2):
    return pl.pallas_call(
        last_body,
        out_shape=jax.ShapeDtypeStruct((OWNERS, 4, 3, ROWS, COLS), BF),
        in_specs=[SM] + [VM] * 9,
        out_specs=HB,
        scratch_shapes=[
            pltpu.VMEM((6 * COLS, NI), F32),
            pltpu.VMEM((3, 4, NI, COLS), BF),
            pltpu.VMEM((6 * COLS, NI), BF),
            pltpu.VMEM((3, OWNERS, 4, ROWS, COLS), BF),
            pltpu.SemaphoreType.DMA((3,)),
        ],
        cost_estimate=cost(2 * KERNEL_FLOPS + 2 * 3 * NI * NI * NI, 8 << 20),
        compiler_params=SMALL,
        name="last_rows",
    )(place, v0, v1, v2, v3, form, turned_form, weights, k0, k2)


def forward_body(terms, matrix, out):
    for c in range(3):
        row = c * ROWS
        halves = [terms[:, row + h : row + h + 16, :].reshape(GROUP * 16, COLS) for h in (0, 16)]
        both = jnp.concatenate(halves, axis=1)
        part = jnp.dot(matrix[...], both, preferred_element_type=F32).astype(BF)
        for half in range(2):
            one = part[:, half * COLS : (half + 1) * COLS].reshape(2 * NB, 16, COLS)
            out[2 * half, :, c] = one[:, :QUARTER]
            out[2 * half + 1, :, c] = one[:, QUARTER:]


BONDS = (2 * NB, 3, QUARTER, COLS)


def forward(terms, matrix):
    return pl.pallas_call(
        forward_body,
        out_shape=jax.ShapeDtypeStruct((4,) + BONDS, BF),
        in_specs=[VM, VM],
        out_specs=VM,
        cost_estimate=cost(2 * 256 * 1024 * 768, 3 << 20),
        compiler_params=SMALL,
        name="forward",
    )(terms, matrix)


def mix_body(parts, matrix, out):
    total = parts[0].astype(F32)
    for k in range(1, 4):
        total += parts[k].astype(F32)
    flat = total.reshape(6 * NB * QUARTER, COLS)
    high = flat.astype(BF)
    rest = flat - high.astype(F32)
    middle = rest.astype(BF)
    low = (rest - middle.astype(F32)).astype(BF)
    split = jnp.concatenate([high, middle, low], axis=1)
    mixed = jnp.dot(matrix[...], split, preferred_element_type=F32)
    mixed = mixed[:, :COLS] + (mixed[:, COLS : 2 * COLS] + mixed[:, 2 * COLS :])
    out[...] = mixed.reshape(BONDS).astype(BF)


def mix(parts, matrix):
    return pl.pallas_call(
        mix_body,
        out_shape=jax.ShapeDtypeStruct(BONDS, BF),
        in_specs=[VM] * 2,
        out_specs=VM,
        cost_estimate=cost(2 * 384 * 384 * 384, 1 << 20),
        compiler_params=SMALL,
        name="mix",
    )(parts, matrix)


def backward_body(parts, terms, matrix, out):
    scale = 1.0 / math.sqrt(NB * SOURCES)
    for c in range(3):
        row = c * ROWS
        halves = [
            jnp.concatenate([parts[2 * h, :, c], parts[2 * h + 1, :, c]], axis=1).reshape(
                2 * NB * 16, COLS
            )
            for h in range(2)
        ]
        back = jnp.dot(
            matrix[...], jnp.concatenate(halves, axis=1), preferred_element_type=F32
        )
        for half in range(2):
            here = row + half * 16
            one = back[:, half * COLS : (half + 1) * COLS].reshape(GROUP, 16, COLS)
            flow = terms[:, here : here + 16, :].astype(F32) + one * scale
            out[:, here : here + 16, :] = flow.astype(BF)


def backward(parts, terms, matrix):
    return pl.pallas_call(
        backward_body,
        out_shape=jax.ShapeDtypeStruct((GROUP, 3 * ROWS, COLS), BF),
        in_specs=[VM] * 3,
        out_specs=VM,
        cost_estimate=cost(2 * 256 * 1024 * 768, 5 << 20),
        compiler_params=SMALL,
        name="backward",
    )(parts, terms, matrix)


def finish_body(pieces, out, held, sems):
    def copy(k):
        c, r = divmod(k, 4)
        return pltpu.make_async_copy(held.at[c, r], out.at[c, r], sems.at[k])

    for k in range(12):
        c, r = divmod(k, 4)
        for w in range(OWNERS):
            held[c, r, w * ROWS : (w + 1) * ROWS, :] = pieces[w, r, c].astype(F32)
        if k > 0:
            copy(k - 1).start()
    copy(11).start()
    for k in range(12):
        copy(k).wait()


def finish(pieces):
    return pl.pallas_call(
        finish_body,
        out_shape=jax.ShapeDtypeStruct((3, 4, NI, COLS), F32),
        in_specs=[VM],
        out_specs=pl.BlockSpec(memory_space=pl.ANY),
        scratch_shapes=[pltpu.VMEM((3, 4, NI, COLS), F32), pltpu.SemaphoreType.DMA((12,))],
        cost_estimate=cost(1 << 20, 5 << 20),
        compiler_params=SMALL,
        name="finish",
    )(pieces)


def turn(value, axis, shift):
    return lax.ppermute(value, axis, [(k, (k + shift) % 4) for k in range(4)])


def local(
    vertex, formfactors, propagator, loop_mom, bond_disp, proj_channel, proj_bond, proj_phase
):
    x = lax.axis_index("x")
    z = lax.axis_index("z4")
    owner = lax.axis_index(("z4", "z2", "y", "c"))
    place_x = jnp.reshape(x, (1,)).astype(jnp.int32)

    sent = {}
    source = vertex
    for s in (2, 1, 3):
        sent[s] = lax.dynamic_index_in_dim(source, (x + s) % 4, 1, keepdims=False)
        source, sent[s] = lax.optimization_barrier((source, sent[s]))
    v2 = turn(sent[2], "x", 2)
    v1 = turn(sent[1], "x", 1)
    v3 = turn(sent[3], "x", 3)

    weights = loop_weights(propagator, loop_mom, 4 * owner + x)
    phases = phase_table(bond_disp, GROUP * z + jnp.arange(GROUP, dtype=jnp.int32))
    there = times_identity(phases, 16).astype(BF)
    back = times_identity(phases.T, 16).astype(BF)
    mixing = mixing_matrix(proj_channel, proj_bond, proj_phase)
    mixing = times_identity(mixing, QUARTER).astype(BF)


    k0, turned_form, v0 = own_rows(place_x, vertex, formfactors, weights)
    k2 = panel_rows(v2, formfactors, turned_form, weights)
    increment = last_rows(
        place_x, v0, v1, v2, v3, formfactors, turned_form, weights, k0, k2
    )
    increment = increment.reshape(GROUP, 3 * ROWS, COLS)
    terms = lax.all_to_all(increment, ("z2", "y", "c", "x"), 0, 0, tiled=True)

    sums = lax.all_to_all(forward(terms, there), "z4", 0, 0, tiled=True)
    parts = lax.all_gather(mix(sums, mixing), "z4", axis=0, tiled=False)
    flow = backward(parts, terms, back)
    flow = flow.reshape(OWNERS, 4 * 3 * ROWS, COLS)
    pieces = lax.all_to_all(flow, ("z2", "y", "c"), 0, 0, tiled=True)
    return finish(pieces.reshape(OWNERS, 4, 3, ROWS, COLS))


def solution(mesh):
    fine = Mesh(mesh.devices.reshape(4, 2, 4, 2, 4), ("z4", "z2", "y", "c", "x"))
    placed = P(None, ("z4", "z2", "y", "c"), None, "x")
    in_specs = (placed, P(), P(), P(), P(), P(), P(), P())
    return jax.shard_map(local, mesh=fine, in_specs=in_specs, out_specs=placed, check_vma=False)
```

```python
import math

import jax
import jax.numpy as jnp
from jax import lax
from jax.experimental import pallas as pl
from jax.experimental.pallas import tpu as pltpu
from jax.sharding import Mesh
from jax.sharding import PartitionSpec as P

MSIDE = 16
NQ = 256
NI = 512
NL = 2048
NB = 8
SOURCES = 4
COLS = 128
GROUP = 64
OWNERS = 16
ROWS = NI // OWNERS
QUARTER = ROWS // 4
LCHUNK = 512


BF = jnp.bfloat16
F32 = jnp.float32


def cost(flops, nbytes):
    return pl.CostEstimate(flops=flops, bytes_accessed=nbytes, transcendentals=0)


def nt_dot(a, b):
    return lax.dot_general(a, b, (((1,), (1,)), ((), ())), preferred_element_type=F32)


def momentum_sum(former, latter, signed):
    coord_x = (former // MSIDE + signed * (latter // MSIDE)) % MSIDE
    coord_y = (former % MSIDE + signed * (latter % MSIDE)) % MSIDE
    return coord_x * MSIDE + coord_y


def lookup(values, indices):
    hits = indices[..., None] == jnp.arange(values.shape[0], dtype=jnp.int32)
    return jnp.sum(jnp.where(hits, values, 0.0), axis=-1)


def loop_weights(propagator, loop_mom, q):
    every = jnp.arange(NQ, dtype=jnp.int32)
    partners = jnp.stack(
        [momentum_sum(q, every, -1), momentum_sum(every, q, 1), momentum_sum(every, q, -1)]
    )
    table = jnp.concatenate([propagator[None, :], lookup(propagator, partners)], axis=0)
    hot = (every[:, None] == loop_mom[None, :]).astype(F32)
    found = jnp.einsum("nk,kl->nl", table, hot, precision=lax.Precision.HIGHEST)
    return found[0:1] * found[1:4] * (1.0 / math.sqrt(NL))


def phase_table(bond_disp, momenta):
    coord_x = momenta // MSIDE
    coord_y = momenta % MSIDE
    turns = (bond_disp[:, 0:1] * coord_x[None, :] + bond_disp[:, 1:2] * coord_y[None, :]) % MSIDE
    angles = turns.astype(F32) * (2.0 * math.pi / MSIDE)
    return jnp.concatenate([jnp.cos(angles), -jnp.sin(angles)], axis=0).astype(BF)


def hot(shape, axis, each):
    long = lax.broadcasted_iota(jnp.int32, shape, axis) // each
    short = lax.broadcasted_iota(jnp.int32, shape, 1 - axis)
    return jnp.where(long == short, 1.0, 0.0).astype(BF)


def times_identity(matrix, each):
    rows, cols = matrix.shape
    wide = jnp.dot(matrix, hot((cols, cols * each), 1, each), preferred_element_type=F32)
    full = jnp.dot(
        hot((rows * each, rows), 0, each), wide.astype(BF), preferred_element_type=F32
    )
    row_id = lax.broadcasted_iota(jnp.int32, full.shape, 0) % each
    col_id = lax.broadcasted_iota(jnp.int32, full.shape, 1) % each
    return jnp.where(row_id == col_id, full, 0.0).astype(BF)


def mixing_matrix(proj_channel, proj_bond, proj_phase):
    chan_hot = (proj_channel[..., None] == jnp.arange(3, dtype=jnp.int32)).astype(F32)
    bond_hot = (proj_bond[..., None] == jnp.arange(NB, dtype=jnp.int32)).astype(F32)
    direct = (proj_phase == 0).astype(F32) - (proj_phase == 2).astype(F32)
    crossed = (proj_phase == 3).astype(F32) - (proj_phase == 1).astype(F32)
    pair = (bond_hot[..., :, None] * chan_hot[..., None, :]).reshape(3, NB, SOURCES, 3 * NB)
    same = jnp.sum(pair * direct[..., None], axis=2)
    swapped = jnp.sum(pair * crossed[..., None], axis=2)
    same = jnp.swapaxes(same, 0, 1).reshape(3 * NB, 3 * NB)
    swapped = jnp.swapaxes(swapped, 0, 1).reshape(3 * NB, 3 * NB)
    upper = jnp.concatenate([same, swapped], axis=1)
    lower = jnp.concatenate([-swapped, same], axis=1)
    return (jnp.concatenate([upper, lower], axis=0) * (1.0 / MSIDE)).astype(BF)


def kernel_rows(panels, form, turned_form, weights, total):
    turned = jnp.concatenate([panel(c).T for panel in panels for c in range(3)], axis=0)
    count = 3 * len(panels)
    for step in range(NL // LCHUNK):
        low, high = step * LCHUNK, (step + 1) * LCHUNK
        terms = jnp.dot(turned, turned_form[:, low:high], preferred_element_type=F32)
        weighted = jnp.concatenate(
            [
                (
                    terms[k * COLS : (k + 1) * COLS] * weights[k % 3 : k % 3 + 1, low:high]
                ).astype(BF)
                for k in range(count)
            ],
            axis=0,
        )
        add = jnp.dot(weighted, form[low:high, :], preferred_element_type=F32)
        if step == 0:
            total[...] = add
        else:
            total[...] += add


def own_body(place, vertex, form, weights, out, turned_form, v0, total, sem):
    own = pltpu.make_async_copy(vertex.at[:, place[0]], v0, sem)
    own.start()
    for step in range(NL // LCHUNK):
        low, high = step * LCHUNK, (step + 1) * LCHUNK
        turned_form[:, low:high] = form[low:high, :].T
    own.wait()
    kernel_rows([lambda c: v0[c]], form, turned_form, weights, total)
    out[...] = total[...].astype(BF)


def panel_body(
    panel, form, turned_form, weights, phases, turned_phases, table, out, there, back, mixing, total
):
    kernel_rows([lambda c: panel[c]], form, turned_form, weights, total)
    out[...] = total[...].astype(BF)
    there[...] = times_identity(phases[...], 16)
    back[...] = times_identity(turned_phases[...], 16)
    mixing[...] = times_identity(table[...], QUARTER)


def last_body(
    place, v0, v1, v2, v3, form, turned_form, weights, k0, k2, out, total, whole, k13
):
    x = place[0]
    kernel_rows([lambda c: v1[c], lambda c: v3[c]], form, turned_form, weights, total)
    k13[...] = total[...].astype(BF)
    for c in range(3):
        for s in range(4):
            whole[c, lax.rem(x + 4 - s, 4)] = (v0, v1, v2, v3)[s][c]

    for c in range(3):
        row = c * COLS
        natural = jnp.concatenate([whole[c, n] for n in range(4)], axis=1)
        rows = jnp.concatenate(
            [
                k0[row : row + COLS],
                k13[row : row + COLS],
                k2[row : row + COLS],
                k13[3 * COLS + row : 3 * COLS + row + COLS],
            ],
            axis=0,
        )
        inc = nt_dot(natural, rows).astype(BF)
        for s in range(4):
            part = inc[:, s * COLS : (s + 1) * COLS].reshape(OWNERS, 1, ROWS, COLS)
            out[:, pl.ds(lax.rem(x + 4 - s, 4), 1), c] = part


VM = pl.BlockSpec(memory_space=pltpu.VMEM)
SMALL = pltpu.CompilerParams(vmem_limit_bytes=24 << 20)
KERNEL_FLOPS = 2 * 2 * 3 * COLS * NL * NI


HB = pl.BlockSpec(memory_space=pltpu.HBM)
SM = pl.BlockSpec(memory_space=pltpu.SMEM)


def own_rows(place, vertex, form, weights):
    return pl.pallas_call(
        own_body,
        out_shape=[
            jax.ShapeDtypeStruct((3 * COLS, NI), BF),
            jax.ShapeDtypeStruct((NI, NL), BF),
            jax.ShapeDtypeStruct((3, NI, COLS), BF),
        ],
        in_specs=[SM, HB, VM, VM],
        out_specs=[VM] * 3,
        scratch_shapes=[pltpu.VMEM((3 * COLS, NI), F32), pltpu.SemaphoreType.DMA],
        cost_estimate=cost(KERNEL_FLOPS, 3 << 20),
        compiler_params=SMALL,
        name="own_rows",
    )(place, vertex, form, weights)


def panel_rows(panel, form, turned_form, weights, phases, turned_phases, table):
    return pl.pallas_call(
        panel_body,
        out_shape=[
            jax.ShapeDtypeStruct((3 * COLS, NI), BF),
            jax.ShapeDtypeStruct((2 * NB * 16, GROUP * 16), BF),
            jax.ShapeDtypeStruct((GROUP * 16, 2 * NB * 16), BF),
            jax.ShapeDtypeStruct((6 * NB * QUARTER, 6 * NB * QUARTER), BF),
        ],
        in_specs=[VM] * 7,
        out_specs=[VM] * 4,
        scratch_shapes=[pltpu.VMEM((3 * COLS, NI), F32)],
        cost_estimate=cost(KERNEL_FLOPS, 3 << 20),
        compiler_params=SMALL,
        name="panel_rows",
    )(panel, form, turned_form, weights, phases, turned_phases, table)


def last_rows(place, v0, v1, v2, v3, form, turned_form, weights, k0, k2):
    return pl.pallas_call(
        last_body,
        out_shape=jax.ShapeDtypeStruct((OWNERS, 4, 3, ROWS, COLS), BF),
        in_specs=[SM] + [VM] * 9,
        out_specs=VM,
        scratch_shapes=[
            pltpu.VMEM((6 * COLS, NI), F32),
            pltpu.VMEM((3, 4, NI, COLS), BF),
            pltpu.VMEM((6 * COLS, NI), BF),
        ],
        cost_estimate=cost(2 * KERNEL_FLOPS + 2 * 3 * NI * NI * NI, 8 << 20),
        compiler_params=SMALL,
        name="last_rows",
    )(place, v0, v1, v2, v3, form, turned_form, weights, k0, k2)


def forward_body(terms, matrix, out):
    for c in range(3):
        row = c * ROWS
        halves = [terms[:, row + h : row + h + 16, :].reshape(GROUP * 16, COLS) for h in (0, 16)]
        both = jnp.concatenate(halves, axis=1)
        part = jnp.dot(matrix[...], both, preferred_element_type=F32).astype(BF)
        for half in range(2):
            one = part[:, half * COLS : (half + 1) * COLS].reshape(2 * NB, 16, COLS)
            out[2 * half, :, c] = one[:, :QUARTER]
            out[2 * half + 1, :, c] = one[:, QUARTER:]


BONDS = (2 * NB, 3, QUARTER, COLS)


def forward(terms, matrix):
    return pl.pallas_call(
        forward_body,
        out_shape=jax.ShapeDtypeStruct((4,) + BONDS, BF),
        in_specs=[VM, VM],
        out_specs=VM,
        cost_estimate=cost(2 * 256 * 1024 * 768, 3 << 20),
        compiler_params=SMALL,
        name="forward",
    )(terms, matrix)


def mix_body(parts, matrix, out):
    total = parts[0].astype(F32)
    for k in range(1, 4):
        total += parts[k].astype(F32)
    flat = total.reshape(6 * NB * QUARTER, COLS)
    high = flat.astype(BF)
    rest = flat - high.astype(F32)
    middle = rest.astype(BF)
    low = (rest - middle.astype(F32)).astype(BF)
    split = jnp.concatenate([high, middle, low], axis=1)
    mixed = jnp.dot(matrix[...], split, preferred_element_type=F32)
    mixed = mixed[:, :COLS] + (mixed[:, COLS : 2 * COLS] + mixed[:, 2 * COLS :])
    out[...] = mixed.reshape(BONDS).astype(BF)


def mix(parts, matrix):
    return pl.pallas_call(
        mix_body,
        out_shape=jax.ShapeDtypeStruct(BONDS, BF),
        in_specs=[VM] * 2,
        out_specs=VM,
        cost_estimate=cost(2 * 384 * 384 * 384, 1 << 20),
        compiler_params=SMALL,
        name="mix",
    )(parts, matrix)


def backward_body(parts, terms, matrix, out):
    scale = 1.0 / math.sqrt(NB * SOURCES)
    for c in range(3):
        row = c * ROWS
        halves = [
            jnp.concatenate([parts[2 * h, :, c], parts[2 * h + 1, :, c]], axis=1).reshape(
                2 * NB * 16, COLS
            )
            for h in range(2)
        ]
        back = jnp.dot(
            matrix[...], jnp.concatenate(halves, axis=1), preferred_element_type=F32
        )
        for half in range(2):
            here = row + half * 16
            one = back[:, half * COLS : (half + 1) * COLS].reshape(GROUP, 16, COLS)
            flow = terms[:, here : here + 16, :].astype(F32) + one * scale
            out[:, here : here + 16, :] = flow.astype(BF)


def backward(parts, terms, matrix):
    return pl.pallas_call(
        backward_body,
        out_shape=jax.ShapeDtypeStruct((GROUP, 3 * ROWS, COLS), BF),
        in_specs=[VM] * 3,
        out_specs=VM,
        cost_estimate=cost(2 * 256 * 1024 * 768, 5 << 20),
        compiler_params=SMALL,
        name="backward",
    )(parts, terms, matrix)


def finish_body(pieces, out, held, sems):
    def copy(k):
        c, r = divmod(k, 4)
        return pltpu.make_async_copy(held.at[c, r], out.at[c, r], sems.at[k])

    for k in range(12):
        c, r = divmod(k, 4)
        for w in range(OWNERS):
            held[c, r, w * ROWS : (w + 1) * ROWS, :] = pieces[w, r, c].astype(F32)
        if k > 0:
            copy(k - 1).start()
    copy(11).start()
    for k in range(12):
        copy(k).wait()


def finish(pieces):
    return pl.pallas_call(
        finish_body,
        out_shape=jax.ShapeDtypeStruct((3, 4, NI, COLS), F32),
        in_specs=[VM],
        out_specs=pl.BlockSpec(memory_space=pl.ANY),
        scratch_shapes=[pltpu.VMEM((3, 4, NI, COLS), F32), pltpu.SemaphoreType.DMA((12,))],
        cost_estimate=cost(1 << 20, 5 << 20),
        compiler_params=SMALL,
        name="finish",
    )(pieces)


def turn(value, axis, shift):
    return lax.ppermute(value, axis, [(k, (k + shift) % 4) for k in range(4)])


def local(
    vertex, formfactors, propagator, loop_mom, bond_disp, proj_channel, proj_bond, proj_phase
):
    x = lax.axis_index("x")
    z = lax.axis_index("z4")
    owner = lax.axis_index(("z4", "z2", "y", "c"))
    place_x = jnp.reshape(x, (1,)).astype(jnp.int32)

    sent = {}
    source = vertex
    for s in (2, 1, 3):
        sent[s] = lax.dynamic_index_in_dim(source, (x + s) % 4, 1, keepdims=False)
        source, sent[s] = lax.optimization_barrier((source, sent[s]))
    v2 = turn(sent[2], "x", 2)
    v1 = turn(sent[1], "x", 1)
    v3 = turn(sent[3], "x", 3)

    weights = loop_weights(propagator, loop_mom, 4 * owner + x)
    phases = phase_table(bond_disp, GROUP * z + jnp.arange(GROUP, dtype=jnp.int32))
    table = mixing_matrix(proj_channel, proj_bond, proj_phase)

    k0, turned_form, v0 = own_rows(place_x, vertex, formfactors, weights)
    k2, there, back, mixing = panel_rows(
        v2, formfactors, turned_form, weights, phases, phases.T, table
    )
    increment = last_rows(
        place_x, v0, v1, v2, v3, formfactors, turned_form, weights, k0, k2
    )
    increment = increment.reshape(GROUP, 3 * ROWS, COLS)
    terms = lax.all_to_all(increment, ("z2", "y", "c", "x"), 0, 0, tiled=True)

    sums = lax.all_to_all(forward(terms, there), "z4", 0, 0, tiled=True)
    parts = lax.all_gather(mix(sums, mixing), "z4", axis=0, tiled=False)
    flow = backward(parts, terms, back)
    flow = flow.reshape(OWNERS, 4 * 3 * ROWS, COLS)
    pieces = lax.all_to_all(flow, ("z2", "y", "c"), 0, 0, tiled=True)
    return finish(pieces.reshape(OWNERS, 4, 3, ROWS, COLS))


def solution(mesh):
    fine = Mesh(mesh.devices.reshape(4, 2, 4, 2, 4), ("z4", "z2", "y", "c", "x"))
    placed = P(None, ("z4", "z2", "y", "c"), None, "x")
    in_specs = (placed, P(), P(), P(), P(), P(), P(), P())
    return jax.shard_map(local, mesh=fine, in_specs=in_specs, out_specs=placed, check_vma=False)
```

```python
import math

import jax
import jax.numpy as jnp
from jax import lax
from jax.experimental import pallas as pl
from jax.experimental.pallas import tpu as pltpu
from jax.sharding import Mesh
from jax.sharding import PartitionSpec as P

MSIDE = 16
NQ = 256
NI = 512
NL = 2048
NB = 8
SOURCES = 4
COLS = 128
GROUP = 64
OWNERS = 16
ROWS = NI // OWNERS
QUARTER = ROWS // 4
LCHUNK = 1024


BF = jnp.bfloat16
F32 = jnp.float32


def cost(flops, nbytes):
    return pl.CostEstimate(flops=flops, bytes_accessed=nbytes, transcendentals=0)


def nt_dot(a, b):
    return lax.dot_general(a, b, (((1,), (1,)), ((), ())), preferred_element_type=F32)


def momentum_sum(former, latter, signed):
    coord_x = (former // MSIDE + signed * (latter // MSIDE)) % MSIDE
    coord_y = (former % MSIDE + signed * (latter % MSIDE)) % MSIDE
    return coord_x * MSIDE + coord_y


def lookup(values, indices):
    hits = indices[..., None] == jnp.arange(values.shape[0], dtype=jnp.int32)
    return jnp.sum(jnp.where(hits, values, 0.0), axis=-1)


def loop_weights(propagator, loop_mom, q):
    every = jnp.arange(NQ, dtype=jnp.int32)
    partners = jnp.stack(
        [momentum_sum(q, every, -1), momentum_sum(every, q, 1), momentum_sum(every, q, -1)]
    )
    table = jnp.concatenate([propagator[None, :], lookup(propagator, partners)], axis=0)
    hot = (every[:, None] == loop_mom[None, :]).astype(F32)
    found = jnp.einsum("nk,kl->nl", table, hot, precision=lax.Precision.HIGHEST)
    return found[0:1] * found[1:4] * (1.0 / math.sqrt(NL))


def phase_table(bond_disp, momenta):
    coord_x = momenta // MSIDE
    coord_y = momenta % MSIDE
    turns = (bond_disp[:, 0:1] * coord_x[None, :] + bond_disp[:, 1:2] * coord_y[None, :]) % MSIDE
    angles = turns.astype(F32) * (2.0 * math.pi / MSIDE)
    return jnp.concatenate([jnp.cos(angles), -jnp.sin(angles)], axis=0).astype(BF)


def hot(shape, axis, each):
    long = lax.broadcasted_iota(jnp.int32, shape, axis) // each
    short = lax.broadcasted_iota(jnp.int32, shape, 1 - axis)
    return jnp.where(long == short, 1.0, 0.0).astype(BF)


def times_identity(matrix, each):
    rows, cols = matrix.shape
    wide = jnp.dot(matrix, hot((cols, cols * each), 1, each), preferred_element_type=F32)
    full = jnp.dot(
        hot((rows * each, rows), 0, each), wide.astype(BF), preferred_element_type=F32
    )
    row_id = lax.broadcasted_iota(jnp.int32, full.shape, 0) % each
    col_id = lax.broadcasted_iota(jnp.int32, full.shape, 1) % each
    return jnp.where(row_id == col_id, full, 0.0).astype(BF)


def mixing_matrix(proj_channel, proj_bond, proj_phase):
    chan_hot = (proj_channel[..., None] == jnp.arange(3, dtype=jnp.int32)).astype(F32)
    bond_hot = (proj_bond[..., None] == jnp.arange(NB, dtype=jnp.int32)).astype(F32)
    direct = (proj_phase == 0).astype(F32) - (proj_phase == 2).astype(F32)
    crossed = (proj_phase == 3).astype(F32) - (proj_phase == 1).astype(F32)
    pair = (bond_hot[..., :, None] * chan_hot[..., None, :]).reshape(3, NB, SOURCES, 3 * NB)
    same = jnp.sum(pair * direct[..., None], axis=2)
    swapped = jnp.sum(pair * crossed[..., None], axis=2)
    same = jnp.swapaxes(same, 0, 1).reshape(3 * NB, 3 * NB)
    swapped = jnp.swapaxes(swapped, 0, 1).reshape(3 * NB, 3 * NB)
    upper = jnp.concatenate([same, swapped], axis=1)
    lower = jnp.concatenate([-swapped, same], axis=1)
    return (jnp.concatenate([upper, lower], axis=0) * (1.0 / MSIDE)).astype(BF)


def kernel_rows(panels, form, turned_form, weights, total):
    turned = jnp.concatenate([panel(c).T for panel in panels for c in range(3)], axis=0)
    count = 3 * len(panels)
    for step in range(NL // LCHUNK):
        low, high = step * LCHUNK, (step + 1) * LCHUNK
        terms = jnp.dot(turned, turned_form[:, low:high], preferred_element_type=F32)
        weighted = jnp.concatenate(
            [
                (
                    terms[k * COLS : (k + 1) * COLS] * weights[k % 3 : k % 3 + 1, low:high]
                ).astype(BF)
                for k in range(count)
            ],
            axis=0,
        )
        add = jnp.dot(weighted, form[low:high, :], preferred_element_type=F32)
        if step == 0:
            total[...] = add
        else:
            total[...] += add


def own_body(place, vertex, form, weights, out, turned_form, v0, total, sem):
    own = pltpu.make_async_copy(vertex.at[:, place[0]], v0, sem)
    own.start()
    for step in range(NL // LCHUNK):
        low, high = step * LCHUNK, (step + 1) * LCHUNK
        turned_form[:, low:high] = form[low:high, :].T
    own.wait()
    kernel_rows([lambda c: v0[c]], form, turned_form, weights, total)
    out[...] = total[...].astype(BF)


def panel_body(
    panel, form, turned_form, weights, phases, turned_phases, table, out, there, back, mixing, total
):
    kernel_rows([lambda c: panel[c]], form, turned_form, weights, total)
    out[...] = total[...].astype(BF)
    there[...] = times_identity(phases[...], 16)
    back[...] = times_identity(turned_phases[...], 16)
    mixing[...] = times_identity(table[...], QUARTER)


def last_body(
    place, v0, v1, v2, v3, form, turned_form, weights, k0, k2, out, total, whole, k13
):
    x = place[0]
    kernel_rows([lambda c: v1[c], lambda c: v3[c]], form, turned_form, weights, total)
    k13[...] = total[...].astype(BF)
    for c in range(3):
        for s in range(4):
            whole[c, lax.rem(x + 4 - s, 4)] = (v0, v1, v2, v3)[s][c]

    for c in range(3):
        row = c * COLS
        natural = jnp.concatenate([whole[c, n] for n in range(4)], axis=1)
        rows = jnp.concatenate(
            [
                k0[row : row + COLS],
                k13[row : row + COLS],
                k2[row : row + COLS],
                k13[3 * COLS + row : 3 * COLS + row + COLS],
            ],
            axis=0,
        )
        inc = nt_dot(natural, rows).astype(BF)
        for s in range(4):
            part = inc[:, s * COLS : (s + 1) * COLS].reshape(OWNERS, 1, ROWS, COLS)
            out[:, pl.ds(lax.rem(x + 4 - s, 4), 1), c] = part


VM = pl.BlockSpec(memory_space=pltpu.VMEM)
SMALL = pltpu.CompilerParams(vmem_limit_bytes=24 << 20)
KERNEL_FLOPS = 2 * 2 * 3 * COLS * NL * NI


HB = pl.BlockSpec(memory_space=pltpu.HBM)
SM = pl.BlockSpec(memory_space=pltpu.SMEM)


def own_rows(place, vertex, form, weights):
    return pl.pallas_call(
        own_body,
        out_shape=[
            jax.ShapeDtypeStruct((3 * COLS, NI), BF),
            jax.ShapeDtypeStruct((NI, NL), BF),
            jax.ShapeDtypeStruct((3, NI, COLS), BF),
        ],
        in_specs=[SM, HB, VM, VM],
        out_specs=[VM] * 3,
        scratch_shapes=[pltpu.VMEM((3 * COLS, NI), F32), pltpu.SemaphoreType.DMA],
        cost_estimate=cost(KERNEL_FLOPS, 3 << 20),
        compiler_params=SMALL,
        name="own_rows",
    )(place, vertex, form, weights)


def panel_rows(panel, form, turned_form, weights, phases, turned_phases, table):
    return pl.pallas_call(
        panel_body,
        out_shape=[
            jax.ShapeDtypeStruct((3 * COLS, NI), BF),
            jax.ShapeDtypeStruct((2 * NB * 16, GROUP * 16), BF),
            jax.ShapeDtypeStruct((GROUP * 16, 2 * NB * 16), BF),
            jax.ShapeDtypeStruct((6 * NB * QUARTER, 6 * NB * QUARTER), BF),
        ],
        in_specs=[VM] * 7,
        out_specs=[VM] * 4,
        scratch_shapes=[pltpu.VMEM((3 * COLS, NI), F32)],
        cost_estimate=cost(KERNEL_FLOPS, 3 << 20),
        compiler_params=SMALL,
        name="panel_rows",
    )(panel, form, turned_form, weights, phases, turned_phases, table)


def last_rows(place, v0, v1, v2, v3, form, turned_form, weights, k0, k2):
    return pl.pallas_call(
        last_body,
        out_shape=jax.ShapeDtypeStruct((OWNERS, 4, 3, ROWS, COLS), BF),
        in_specs=[SM] + [VM] * 9,
        out_specs=VM,
        scratch_shapes=[
            pltpu.VMEM((6 * COLS, NI), F32),
            pltpu.VMEM((3, 4, NI, COLS), BF),
            pltpu.VMEM((6 * COLS, NI), BF),
        ],
        cost_estimate=cost(2 * KERNEL_FLOPS + 2 * 3 * NI * NI * NI, 8 << 20),
        compiler_params=SMALL,
        name="last_rows",
    )(place, v0, v1, v2, v3, form, turned_form, weights, k0, k2)


def forward_body(place, terms, matrix, *refs):
    outs, held = refs[:4], refs[4]
    for c in range(3):
        row = c * ROWS
        halves = [terms[:, row + h : row + h + 16, :].reshape(GROUP * 16, COLS) for h in (0, 16)]
        both = jnp.concatenate(halves, axis=1)
        part = jnp.dot(matrix[...], both, preferred_element_type=F32).astype(BF)
        for half in range(2):
            one = part[:, half * COLS : (half + 1) * COLS].reshape(2 * NB, 16, COLS)
            held[2 * half, :, c] = one[:, :QUARTER]
            held[2 * half + 1, :, c] = one[:, QUARTER:]
    for s in range(4):
        outs[s][...] = held[lax.rem(place[0] + s, 4)]


BONDS = (2 * NB, 3, QUARTER, COLS)


def forward(place, terms, matrix):
    return pl.pallas_call(
        forward_body,
        out_shape=[jax.ShapeDtypeStruct(BONDS, BF)] * 4,
        in_specs=[SM, VM, VM],
        out_specs=[VM] * 4,
        scratch_shapes=[pltpu.VMEM((4,) + BONDS, BF)],
        cost_estimate=cost(2 * 256 * 1024 * 768, 3 << 20),
        compiler_params=SMALL,
        name="forward",
    )(place, terms, matrix)


def mix_body(p0, p1, p2, p3, matrix, out):
    total = p0[...].astype(F32) + p1[...].astype(F32) + p2[...].astype(F32) + p3[...].astype(F32)
    flat = total.reshape(6 * NB * QUARTER, COLS)
    high = flat.astype(BF)
    rest = flat - high.astype(F32)
    middle = rest.astype(BF)
    low = (rest - middle.astype(F32)).astype(BF)
    split = jnp.concatenate([high, middle, low], axis=1)
    mixed = jnp.dot(matrix[...], split, preferred_element_type=F32)
    mixed = mixed[:, :COLS] + (mixed[:, COLS : 2 * COLS] + mixed[:, 2 * COLS :])
    out[...] = mixed.reshape(BONDS).astype(BF)


def mix(parts, matrix):
    return pl.pallas_call(
        mix_body,
        out_shape=jax.ShapeDtypeStruct(BONDS, BF),
        in_specs=[VM] * 5,
        out_specs=VM,
        cost_estimate=cost(2 * 384 * 384 * 384, 1 << 20),
        compiler_params=SMALL,
        name="mix",
    )(*parts, matrix)


def backward_body(place, p0, p1, p2, p3, terms, matrix, out, parts):
    for s, part in enumerate((p0, p1, p2, p3)):
        parts[lax.rem(place[0] + 4 - s, 4)] = part[...]
    scale = 1.0 / math.sqrt(NB * SOURCES)
    for c in range(3):
        row = c * ROWS
        halves = [
            jnp.concatenate([parts[2 * h, :, c], parts[2 * h + 1, :, c]], axis=1).reshape(
                2 * NB * 16, COLS
            )
            for h in range(2)
        ]
        back = jnp.dot(
            matrix[...], jnp.concatenate(halves, axis=1), preferred_element_type=F32
        )
        for half in range(2):
            here = row + half * 16
            one = back[:, half * COLS : (half + 1) * COLS].reshape(GROUP, 16, COLS)
            flow = terms[:, here : here + 16, :].astype(F32) + one * scale
            out[:, here : here + 16, :] = flow.astype(BF)


def backward(place, parts, terms, matrix):
    return pl.pallas_call(
        backward_body,
        out_shape=jax.ShapeDtypeStruct((GROUP, 3 * ROWS, COLS), BF),
        in_specs=[SM] + [VM] * 6,
        out_specs=VM,
        scratch_shapes=[pltpu.VMEM((4,) + BONDS, BF)],
        cost_estimate=cost(2 * 256 * 1024 * 768, 5 << 20),
        compiler_params=SMALL,
        name="backward",
    )(place, *parts, terms, matrix)


def finish_body(pieces, out, held, sems):
    def copy(k):
        c, r = divmod(k, 4)
        return pltpu.make_async_copy(held.at[c, r], out.at[c, r], sems.at[k])

    for k in range(12):
        c, r = divmod(k, 4)
        for w in range(OWNERS):
            held[c, r, w * ROWS : (w + 1) * ROWS, :] = pieces[w, r, c].astype(F32)
        if k > 0:
            copy(k - 1).start()
    copy(11).start()
    for k in range(12):
        copy(k).wait()


def finish(pieces):
    return pl.pallas_call(
        finish_body,
        out_shape=jax.ShapeDtypeStruct((3, 4, NI, COLS), F32),
        in_specs=[VM],
        out_specs=pl.BlockSpec(memory_space=pl.ANY),
        scratch_shapes=[pltpu.VMEM((3, 4, NI, COLS), F32), pltpu.SemaphoreType.DMA((12,))],
        cost_estimate=cost(1 << 20, 5 << 20),
        compiler_params=SMALL,
        name="finish",
    )(pieces)


def turn(value, axis, shift):
    return lax.ppermute(value, axis, [(k, (k + shift) % 4) for k in range(4)])


def local(
    vertex, formfactors, propagator, loop_mom, bond_disp, proj_channel, proj_bond, proj_phase
):
    x = lax.axis_index("x")
    z = lax.axis_index("z4")
    owner = lax.axis_index(("z4", "z2", "y", "c"))
    place_x = jnp.reshape(x, (1,)).astype(jnp.int32)
    place_z = jnp.reshape(z, (1,)).astype(jnp.int32)

    sent = {}
    source = vertex
    for s in (2, 1, 3):
        sent[s] = lax.dynamic_index_in_dim(source, (x + s) % 4, 1, keepdims=False)
        source, sent[s] = lax.optimization_barrier((source, sent[s]))
    v2 = turn(sent[2], "x", 2)
    v1 = turn(sent[1], "x", 1)
    v3 = turn(sent[3], "x", 3)

    weights = loop_weights(propagator, loop_mom, 4 * owner + x)
    phases = phase_table(bond_disp, GROUP * z + jnp.arange(GROUP, dtype=jnp.int32))
    table = mixing_matrix(proj_channel, proj_bond, proj_phase)

    k0, turned_form, v0 = own_rows(place_x, vertex, formfactors, weights)
    k2, there, back, mixing = panel_rows(
        v2, formfactors, turned_form, weights, phases, phases.T, table
    )
    increment = last_rows(
        place_x, v0, v1, v2, v3, formfactors, turned_form, weights, k0, k2
    )
    increment = increment.reshape(GROUP, 3 * ROWS, COLS)
    terms = lax.all_to_all(increment, ("z2", "y", "c", "x"), 0, 0, tiled=True)

    sums = forward(place_z, terms, there)
    s2 = turn(sums[2], "z4", 2)
    s1 = turn(sums[1], "z4", 1)
    s3 = turn(sums[3], "z4", 3)
    own = mix((sums[0], s1, s2, s3), mixing)
    b2 = turn(own, "z4", 2)
    b1 = turn(own, "z4", 1)
    b3 = turn(own, "z4", 3)
    flow = backward(place_z, (own, b1, b2, b3), terms, back)
    flow = flow.reshape(OWNERS, 4 * 3 * ROWS, COLS)
    pieces = lax.all_to_all(flow, ("z2", "y", "c"), 0, 0, tiled=True)
    return finish(pieces.reshape(OWNERS, 4, 3, ROWS, COLS))


def solution(mesh):
    fine = Mesh(mesh.devices.reshape(4, 2, 4, 2, 4), ("z4", "z2", "y", "c", "x"))
    placed = P(None, ("z4", "z2", "y", "c"), None, "x")
    in_specs = (placed, P(), P(), P(), P(), P(), P(), P())
    return jax.shard_map(local, mesh=fine, in_specs=in_specs, out_specs=placed, check_vma=False)
```
